32 devices in a mesh: gx: 8 (over z, y), gy: 4 (over x, core).
Axes of the slice: x: 2, y: 2, z: 4, core: 2. Of those that a mesh axis runs over, the one named last changes fastest.
Arguments:
- table: float32 [4, 65536, 128], P(None, 'gx'), may hold values from -2.1 to 2.1
- lookup_owner: int32 [4, 8192, 16, 1], P(None, ('gx', 'gy')), may hold values from 0 to 7; in each aligned block of 4096 rows (0 to 4095, 4096 to 8191, ..., all dimensions but the last counted through in order) at most 1024 rows name the same one
- lookup_row: int32 [4, 8192, 16], P(None, ('gx', 'gy')), may hold values from 0 to 8191
- bag_length: int32 [4, 8192], P(None, ('gx', 'gy')), may hold values from 1 to 16
- top_in: bfloat16 [512, 8192], P(None, 'gy'), may hold values from -0.25 to 0.25
- top_bias: float32 [8192], P('gy'), may hold values from -3 to 3
- top_out: bfloat16 [8192, 1024], P('gy'), may hold values from -0.0625 to 0.0625
Outputs:
- scored: bfloat16 [8192, 1024], P(('gx', 'gy'))
The draws below stay inside these ranges and needn't reach their ends.
Inputs may be any that keep to these rules, and one draw needn't show every extreme that they name: `lookup_owner`: in every aligned block of 4096 entries (the lookups of one table from the samples of one device) no owner is named more than 1024 times; some blocks reach 1024.
All inputs are finite; a program needn't handle non-finite values.
Results may differ from the reference program's by a relative error of at most 0.0057.
Values may be sent and summed in bfloat16 or wider, within the bound.
A program may use at most 128 MiB of HBM per device.

```python
import math
import jax
import jax.numpy as jnp
import numpy as np
from jax import lax

EMB = 128
TABLES = 4
ROWS_DEV = 8192
SAMPLES_DEV = 256
BAG = 16
TOP_W = 8192
OUT_W = 1024
ROWS = 65536
BATCH = 8192
CAP = 1024
N_GX = 8


def set_ends(values, key, smallest, high):
    longest = values.shape.index(max(values.shape))
    spots = []
    for shift in (0, 1):
        where = [jax.random.randint(jax.random.fold_in(key, axis), (), 0, length) for axis, length in enumerate(values.shape)]
        where[longest] = (where[longest] + shift) % values.shape[longest]
        spots.append(tuple(where))
    return values.at[spots[0]].set(smallest).at[spots[1]].set(high)


def levels(stream_key, extent, cuts, low, top_value):
    level, own = 1.0, jax.random.fold_in(stream_key, 6)
    for dim, blocks in cuts:
        steps = jnp.exp(jax.random.uniform(jax.random.fold_in(own, dim), (blocks,), jnp.float32, low / len(cuts), top_value / len(cuts)))
        level = level * jnp.repeat(steps, extent[dim] // blocks).reshape([-1 if axis == dim else 1 for axis in range(len(extent))])
    return level


def rank_bounds(number_of, lean):
    portions = [(1 << 20) // math.isqrt(rank ** lean) + 1 for rank in range(1, number_of + 1)]
    width = 1 + sum(portions) // (1 << 30)
    return np.cumsum(np.array([max(1, weight // width) for weight in portions]))


def ranked_ids(stream_key, extent, number_of, skew):
    table = rank_bounds(number_of, skew)
    pick = jax.random.randint(jax.random.fold_in(stream_key, 1), extent, 0, int(table[number_of - 1]))
    rank = jnp.searchsorted(jnp.asarray(table, jnp.int32), pick, side="right")
    return jax.random.permutation(jax.random.fold_in(stream_key, 2), number_of)[rank].astype(jnp.int32)


def deal_out(stream_key, own, number, rows, number_of, top, most, slope):
    sequence = jax.random.permutation(stream_key, number_of)
    crowded, common = portions_of(number_of, rows * top, most, slope, True), portions_of(number_of, rows * top, most, slope, False)
    places = jnp.arange(number_of)

    def named(tallies, turn):
        used = int((tallies > 0).sum())
        fixed = max(1, used // 4)
        passed = fixed + (places - fixed + turn * (used - fixed)) % max(1, number_of - fixed)
        return jnp.zeros((number_of,), jnp.int32).at[sequence[jnp.where(places < fixed, places, passed)]].set(jnp.asarray(tallies, jnp.int32))

    tallies = jnp.where(number % 4 == 0, named(crowded, number // 4), named(common, number - number // 4 - 1))
    mixed = jax.random.permutation(jax.random.fold_in(own, 3), number_of)
    donor, receiver = mixed[0:number_of // 2 * 2:2], mixed[1:number_of // 2 * 2:2]
    margin = jnp.minimum(tallies[donor] - 1, most - tallies[receiver]) // 2
    margin = jnp.where((donor == sequence[0]) | (receiver == sequence[0]) | (tallies[receiver] == 0), 0, jnp.maximum(margin, 0))
    passed = jax.random.randint(jax.random.fold_in(own, 4), (number_of // 2,), 0, 1 << 20) % (margin + 1)
    tallies = tallies.at[donor].add(-passed).at[receiver].add(passed)
    labels = jnp.searchsorted(jnp.cumsum(tallies), jnp.arange(rows * top), side="right").astype(jnp.int32)
    table = labels.reshape(top, rows).T
    table = table[jax.random.permutation(jax.random.fold_in(own, 1), rows)]
    turn = jax.random.randint(jax.random.fold_in(own, 2), (rows, 1), 0, top)
    return jnp.take_along_axis(table, (jnp.arange(top)[None, :] + turn) % top, axis=1)


def portions_of(amount, total, reach, skew, full):
    weights = [(1 << 20) // math.isqrt(rank ** skew) + 1 for rank in range(1, amount + 1)]
    largest = reach if full else min(reach, max(-(-total // amount), total * weights[0] // sum(weights)))
    least = 1 if total - largest >= amount - 1 else 0
    counts, rest = [largest] + [least] * (amount - 1), total - largest - least * (amount - 1)
    while rest > 0:
        free = [i for i in range(1, amount) if counts[i] < largest] or [i for i in range(1, amount) if counts[i] < reach]
        pool, budget = sum([weights[i] for i in free]), rest
        for i in free:
            extra = min(reach - counts[i], max(1, budget * weights[i] // pool), rest)
            counts[i] = counts[i] + extra
            rest = rest - extra
    return np.array(counts)


def noise(rng, shape, deviation, bound, split=(), kind=jnp.bfloat16):
    drawn = jax.random.normal(rng, shape, jnp.float32) * deviation
    if len(split) > 0:
        drawn = levels(rng, shape, split, -0.22, 0.18) * drawn
    return jnp.clip(drawn, min=-bound, max=bound).astype(kind)


def setup_inputs(seed: int = 0) -> dict:
    seeds = jax.random.split(jax.random.key(seed), 8)
    table = noise(seeds[0], (TABLES, ROWS, EMB), 0.35, 2.1, ((1, 8),), jnp.float32)
    lookup_owner_keys = jax.random.split(jax.random.fold_in(seeds[1], 1), TABLES * BATCH * BAG // (SAMPLES_DEV * BAG))
    lookup_owner_turns = jax.random.permutation(jax.random.fold_in(seeds[1], 3), TABLES * BATCH * BAG // (SAMPLES_DEV * BAG))
    lookup_owner = jax.vmap(lambda own, number: deal_out(jax.random.fold_in(seeds[1], 2), own, number, SAMPLES_DEV * BAG, N_GX, 1, CAP, 1))(lookup_owner_keys, lookup_owner_turns).reshape((TABLES, BATCH, BAG, 1))
    lookup_row = set_ends(ranked_ids(seeds[2], (TABLES, BATCH, BAG), ROWS_DEV, 2), jax.random.fold_in(seeds[2], 3), 0, ROWS_DEV - 1).astype(jnp.int32)
    bag_length = set_ends(jax.random.randint(seeds[3], (TABLES, BATCH), 1, BAG + 1), jax.random.fold_in(seeds[3], 1), 1, BAG).astype(jnp.int32)
    top_in = noise(seeds[4], (TABLES * EMB, TOP_W), (TABLES * EMB) ** -0.5, 0.25, ((1, 4),))
    top_bias = noise(seeds[5], (TOP_W,), 0.5, 3.0, ((0, 4),), jnp.float32)
    top_out = noise(seeds[6], (TOP_W, OUT_W), TOP_W ** -0.5, 0.0625, ((0, 4),))
    return dict(table=table, lookup_owner=lookup_owner, lookup_row=lookup_row, bag_length=bag_length, top_in=top_in, top_bias=top_bias, top_out=top_out)


def pool_table(pieces):
    table_part, index_part, live_part = pieces
    fetched = jnp.take(table_part, index_part, axis=0)
    return jnp.sum(jnp.where(live_part[..., None], fetched, jnp.float32(0.0)), axis=1)


def reference(table, lookup_owner, lookup_row, bag_length, top_in, top_bias, top_out):
    row_index = (lookup_owner[..., 0] * ROWS_DEV + lookup_row).astype(jnp.int32)
    is_live = jnp.arange(BAG, dtype=jnp.int32)[None, None, :] < bag_length[:, :, None]
    pooled = lax.map(pool_table, (table, row_index, is_live))
    features = jnp.transpose(pooled, (1, 0, 2)).reshape(BATCH, TABLES * EMB).astype(jnp.bfloat16)
    blocks = features.reshape(N_GX, BATCH // N_GX, TABLES * EMB)

    def one_block(block):
        pre_act = jnp.dot(block, top_in, preferred_element_type=jnp.float32) + top_bias
        hidden_rows = jnp.maximum(pre_act, 0.0).astype(jnp.bfloat16)
        return jnp.dot(hidden_rows, top_out, preferred_element_type=jnp.float32).astype(jnp.bfloat16)

    scored = lax.map(one_block, blocks)
    return scored.reshape(BATCH, OUT_W)
```

```python
import functools
import jax
import jax.numpy as jnp
from jax import lax
from jax.experimental import pallas as pl
from jax.experimental.pallas import tpu as pltpu
from jax.sharding import PartitionSpec as P

UNROLL = 4
CHAINS = 4
BIG = 2**31 - 1


def log2(n):
    return n.bit_length() - 1


def sort_kernel(rows_dev, owner_ref, row_ref, bag_ref, out_ref):
    tables, bag_size, samples = owner_ref.shape
    owner = owner_ref[...]
    slot = lax.broadcasted_iota(jnp.int32, owner.shape, 1)
    sample = lax.broadcasted_iota(jnp.int32, owner.shape, 2)
    live = slot < bag_ref[...]
    key = jnp.where(live, (owner * samples + sample) * rows_dev + row_ref[...], BIG)
    count = bag_size * samples
    groups = count // 1024
    parts = []
    for t in range(tables):
        for c in range(samples // 128):
            for r in range(bag_size // 8):
                parts.append(key[t, r * 8 : r * 8 + 8, c * 128 : c * 128 + 128])
    lane = lax.broadcasted_iota(jnp.int32, (8, 128), 1)
    sub = lax.broadcasted_iota(jnp.int32, (8, 128), 0)
    place = sub * 128 + lane
    bits = log2(count)
    for k in range(1, bits + 1):
        for j in range(k - 1, -1, -1):
            d = 1 << j
            new = [None] * len(parts)
            for v in range(len(parts)):
                g = v % groups
                if d >= 1024:
                    gd = d // 1024
                    if g & gd:
                        continue
                    w = v + gd
                    low = jnp.minimum(parts[v], parts[w])
                    high = jnp.maximum(parts[v], parts[w])
                    up = ((g * 1024) >> k) & 1 == 0
                    new[v], new[w] = (low, high) if up else (high, low)
                    continue
                x = parts[v]
                if d < 128:
                    a, b = pltpu.roll(x, 128 - d, 1), pltpu.roll(x, d, 1)
                else:
                    s = d // 128
                    a, b = pltpu.roll(x, 8 - s, 0), pltpu.roll(x, s, 0)
                first = (place & d) == 0
                other = jnp.where(first, a, b)
                if (1 << k) >= 1024:
                    up = ((g * 1024) >> k) & 1 == 0
                    take_low = first if up else jnp.logical_not(first)
                else:
                    take_low = ((place >> k) ^ (place >> j)) & 1 == 0
                new[v] = jnp.where(take_low, jnp.minimum(x, other), jnp.maximum(x, other))
            parts = new
    for v in range(len(parts)):
        out_ref[v * 8 : v * 8 + 8, :] = parts[v]


def pool_kernel(samples, count, window, lo_ref, n_ref, keys_ref, table_ref, out_ref, tab, acc, smem, tsem, ksem):
    tables, rows_dev, emb = table_ref.shape
    sources = out_ref.shape[0]
    mask = rows_dev - 1
    shift = log2(rows_dev)
    segs = sources * tables

    def table_copy(t):
        return pltpu.make_async_copy(table_ref.at[t], tab.at[t % 2], tsem.at[t % 2])

    def key_copy(s, t, slot):
        start = lo_ref[s, t] // 1024 * 1024
        start = jnp.minimum(start, count - window)
        src = keys_ref.at[pl.ds(pl.multiple_of((s * tables + t) * count + start, 1024), window)]
        dst = smem.at[pl.ds(slot * window, window)]
        return pltpu.make_async_copy(src, dst, ksem.at[slot])

    steps = [(t, g) for t in range(tables) for g in range(sources // CHAINS)]

    def start_keys(index):
        t, g = steps[index]
        for j in range(CHAINS):
            key_copy(g * CHAINS + j, t, index % 2 * CHAINS + j).start()

    table_copy(0).start()
    start_keys(0)
    for index, (t, g) in enumerate(steps):
        if g == 0:
            if t + 1 < tables:
                table_copy(t + 1).start()
            table_copy(t).wait()
        if index + 1 < len(steps):
            start_keys(index + 1)
        acc[...] = jnp.zeros_like(acc)
        bases, longest = [], 0
        for j in range(CHAINS):
            s = g * CHAINS + j
            slot = index % 2 * CHAINS + j
            key_copy(s, t, slot).wait()
            start = jnp.minimum(lo_ref[s, t] // 1024 * 1024, count - window)
            bases.append(slot * window + lo_ref[s, t] - start)
            longest = jnp.maximum(longest, n_ref[s, t])
        limits = [slot_end for slot_end in range(CHAINS)]
        del limits

        def body(i, carry):
            prevs, runs = list(carry[0]), list(carry[1])
            for u in range(UNROLL):
                for j in range(CHAINS):
                    at = jnp.minimum(bases[j] + i * UNROLL + u, (index % 2 * CHAINS + j + 1) * window - 1)
                    code = smem[at]
                    valid = i * UNROLL + u < n_ref[g * CHAINS + j, t]
                    bag = jnp.where(valid, (code >> shift) & (samples - 1), samples)
                    row = code & mask
                    got = tab[t % 2, pl.ds(row, 1), :]
                    runs[j] = jnp.where(bag == prevs[j], runs[j], 0.0) + got
                    acc[pl.ds(j * (samples + 8) + bag, 1), :] = runs[j]
                    prevs[j] = bag
            return tuple(prevs), tuple(runs)

        init = (
            tuple(jnp.int32(-1) for _ in range(CHAINS)),
            tuple(jnp.zeros((1, emb), jnp.float32) for _ in range(CHAINS)),
        )
        lax.fori_loop(0, (longest + UNROLL - 1) // UNROLL, body, init)
        for j in range(CHAINS):
            out_ref[g * CHAINS + j, :, t * emb : (t + 1) * emb] = acc[
                j * (samples + 8) : j * (samples + 8) + samples, :
            ].astype(out_ref.dtype)


def local(table, lookup_owner, lookup_row, bag_length, top_in, top_bias, top_out):
    owners = lax.axis_size("gx")
    me = lax.axis_index("gx")
    tables, samples, bag_size = lookup_row.shape
    rows_dev = table.shape[1]
    emb = table.shape[2]
    count = samples * bag_size
    cap = 2 * count // owners
    window = min(count, -(-cap // 1024) * 1024 + 1024)

    keys = pl.pallas_call(
        functools.partial(sort_kernel, rows_dev),
        out_shape=jax.ShapeDtypeStruct((tables * count // 128, 128), jnp.int32),
        name="sort_keys",
    )(
        jnp.transpose(lookup_owner[..., 0], (0, 2, 1)),
        jnp.transpose(lookup_row, (0, 2, 1)),
        bag_length[:, None, :],
    )
    all_keys = lax.all_gather(keys, "gx", axis=0, tiled=True)
    span = samples * rows_dev
    segs = all_keys.reshape(owners, tables, count)
    lo = jnp.sum((segs < me * span).astype(jnp.int32), axis=2)
    hi = jnp.sum((segs < (me + 1) * span).astype(jnp.int32), axis=2)
    partial = pl.pallas_call(
        functools.partial(pool_kernel, samples, count, window),
        out_shape=jax.ShapeDtypeStruct((owners, samples, tables * emb), jnp.bfloat16),
        in_specs=[
            pl.BlockSpec(memory_space=pltpu.SMEM),
            pl.BlockSpec(memory_space=pltpu.SMEM),
            pl.BlockSpec(memory_space=pl.ANY),
            pl.BlockSpec(memory_space=pl.ANY),
        ],
        scratch_shapes=[
            pltpu.VMEM((2, rows_dev, emb), jnp.float32),
            pltpu.VMEM((CHAINS * (samples + 8), emb), jnp.float32),
            pltpu.SMEM((2 * CHAINS * window,), jnp.int32),
            pltpu.SemaphoreType.DMA((2,)),
            pltpu.SemaphoreType.DMA((2 * CHAINS,)),
        ],
        name="pool",
    )(lo, hi - lo, all_keys.reshape(-1), table)
    answer = lax.all_to_all(partial, "gx", split_axis=0, concat_axis=0, tiled=True)
    features = jnp.sum(answer.astype(jnp.float32), axis=0).astype(jnp.bfloat16)
    pre_act = (
        jnp.dot(
            lax.all_gather(features, "gy", axis=0, tiled=True),
            top_in,
            preferred_element_type=jnp.float32,
        )
        + top_bias
    )
    hidden_rows = jnp.maximum(pre_act, 0.0).astype(jnp.bfloat16)
    return lax.psum_scatter(
        jnp.dot(hidden_rows, top_out, preferred_element_type=jnp.float32).astype(jnp.bfloat16),
        "gy",
        scatter_dimension=0,
        tiled=True,
    )


def solution(mesh):
    return jax.shard_map(
        local,
        mesh=mesh,
        in_specs=(
            P(None, "gx", None),
            P(None, ("gx", "gy"), None, None),
            P(None, ("gx", "gy"), None),
            P(None, ("gx", "gy")),
            P(None, "gy"),
            P("gy"),
            P("gy", None),
        ),
        out_specs=P(("gx", "gy"), None),
        check_vma=False,
    )
```

```python
import functools
import jax
import jax.numpy as jnp
from jax import lax
from jax.experimental import pallas as pl
from jax.experimental.pallas import tpu as pltpu
from jax.sharding import PartitionSpec as P

UNROLL = 4
CHAINS = 4
BIG = 2**31 - 1
MESH = pl.DeviceIdType.MESH


def log2(n):
    return n.bit_length() - 1


def sort_kernel(rows_dev, owner_ref, row_ref, bag_ref, codes_ref, count_ref, mine, held, send_sem, recv_sem):
    owners = held.shape[0]
    me = lax.axis_index("gx")
    barrier = pltpu.get_barrier_semaphore()
    for k in range(1, owners):
        pl.semaphore_signal(barrier, inc=1, device_id={"gx": lax.rem(me + k, owners)}, device_id_type=MESH)
    tables, bag_size, samples = owner_ref.shape
    owner = owner_ref[...]
    slot = lax.broadcasted_iota(jnp.int32, owner.shape, 1)
    sample = lax.broadcasted_iota(jnp.int32, owner.shape, 2)
    live = slot < bag_ref[...]
    key = jnp.where(live, (owner * samples + sample) * rows_dev + row_ref[...], BIG)
    count = bag_size * samples
    groups = count // 1024
    parts = []
    for t in range(tables):
        for c in range(samples // 128):
            for r in range(bag_size // 8):
                parts.append(key[t, r * 8 : r * 8 + 8, c * 128 : c * 128 + 128])
    lane = lax.broadcasted_iota(jnp.int32, (8, 128), 1)
    sub = lax.broadcasted_iota(jnp.int32, (8, 128), 0)
    place = sub * 128 + lane
    bits = log2(count)
    for k in range(1, bits + 1):
        for j in range(k - 1, -1, -1):
            d = 1 << j
            new = [None] * len(parts)
            for v in range(len(parts)):
                g = v % groups
                if d >= 1024:
                    gd = d // 1024
                    if g & gd:
                        continue
                    w = v + gd
                    low = jnp.minimum(parts[v], parts[w])
                    high = jnp.maximum(parts[v], parts[w])
                    up = ((g * 1024) >> k) & 1 == 0
                    new[v], new[w] = (low, high) if up else (high, low)
                    continue
                x = parts[v]
                if d < 128:
                    a, b = pltpu.roll(x, 128 - d, 1), pltpu.roll(x, d, 1)
                else:
                    s = d // 128
                    a, b = pltpu.roll(x, 8 - s, 0), pltpu.roll(x, s, 0)
                first = (place & d) == 0
                other = jnp.where(first, a, b)
                if (1 << k) >= 1024:
                    up = ((g * 1024) >> k) & 1 == 0
                    take_low = first if up else jnp.logical_not(first)
                else:
                    take_low = ((place >> k) ^ (place >> j)) & 1 == 0
                new[v] = jnp.where(take_low, jnp.minimum(x, other), jnp.maximum(x, other))
            parts = new
    for v in range(len(parts)):
        mine[v * 8 : v * 8 + 8, :] = parts[v]
    pl.semaphore_wait(barrier, owners - 1)
    copies = []
    for k in range(1, owners):
        copies.append(
            pltpu.make_async_remote_copy(
                src_ref=mine,
                dst_ref=held.at[me],
                send_sem=send_sem.at[k],
                recv_sem=recv_sem.at[k],
                device_id={"gx": lax.rem(me + k, owners)},
                device_id_type=MESH,
            )
        )
        copies[-1].start()
    span = samples * rows_dev
    base = me * span

    def recode(source, get):
        for t in range(tables):
            before = jnp.zeros((8, 128), jnp.int32)
            inside = jnp.zeros((8, 128), jnp.int32)
            for g in range(groups):
                at = (t * groups + g) * 8
                x = get(at) - base
                early = x < 0
                ours = jnp.logical_and(x >= 0, x < span)
                codes_ref[source, at : at + 8, :] = jnp.where(ours, x, span)
                before += early.astype(jnp.int32)
                inside += ours.astype(jnp.int32)
            count_ref[0, source, t] = before
            count_ref[1, source, t] = inside

    recode(me, lambda at: mine[at : at + 8, :])
    for k in range(1, owners):
        source = lax.rem(me - k + owners, owners)
        copies[k - 1].wait_recv()
        recode(source, lambda at: held[source, at : at + 8, :])
    for copy in copies:
        copy.wait_send()


def exchange_kernel(part_ref, top_in_ref, bias_ref, top_out_ref, out_ref, from_y, sum_y, from_z, feat, w_in, w_out, hid, near_out, near_in, far_out, w_send, far_in, wsem, ysem, yrec, zsem, zrec, gsem, grec, rsem, rrec, nsem, nrec, fsem, frec):
    owners, samples, width = part_ref.shape
    inner = from_y.shape[0] + 1
    outer = owners // inner
    chips = far_in.shape[0] + 1
    me, mine = lax.axis_index("gx"), lax.axis_index("gy")
    z, y = me // inner, lax.rem(me, inner)
    chip, core = mine // 2, lax.rem(mine, 2)
    partner = chip * 2 + 1 - core
    loads = [
        pltpu.make_async_copy(top_in_ref, w_in, wsem.at[0]),
        pltpu.make_async_copy(top_out_ref, w_out, wsem.at[1]),
    ]
    for load in loads:
        load.start()

    def gx_at(index):
        return {"gx": index}

    def gy_at(index):
        return {"gy": index}

    def remote(src, dst, send, recv, device):
        return pltpu.make_async_remote_copy(
            src_ref=src, dst_ref=dst, send_sem=send, recv_sem=recv, device_id=device, device_id_type=MESH
        )

    def y_at(d):
        return z * inner + lax.rem(y + d, inner)

    def z_at(d):
        return lax.rem(z + d, outer) * inner + y

    def chip_at(d):
        return lax.rem(chip + d, chips) * 2 + core

    peers = [gx_at(y_at(d)) for d in range(1, inner)]
    peers += [gx_at(z_at(d)) for d in range(1, outer)]
    peers += [gy_at(partner)] + [gy_at(chip_at(d)) for d in range(1, chips)]
    barrier = pltpu.get_barrier_semaphore()
    for peer in peers:
        pl.semaphore_signal(barrier, inc=1, device_id=peer, device_id_type=MESH)
    pl.semaphore_wait(barrier, len(peers))

    sends = []
    order = sorted(range(1, outer), key=lambda d: -min(d, outer - d)) + [0]
    y_copies = {}
    for dz in order:
        for d in range(1, inner):
            block = lax.rem(z + dz, outer)
            copy = remote(
                part_ref.at[block * inner + lax.rem(y + d, inner)],
                from_y.at[d - 1, dz],
                ysem.at[d - 1, dz],
                yrec.at[d - 1, dz],
                gx_at(y_at(d)),
            )
            copy.start()
            y_copies[dz, d] = copy
            sends.append(copy)
    step = 64
    z_copies = []
    for dz in order:
        block = lax.rem(z + dz, outer)
        for d in range(1, inner):
            y_copies[dz, d].wait_recv()

        @pl.loop(0, samples // step)
        def _(i):
            rows = pl.ds(pl.multiple_of(i * step, step), step)
            total = part_ref[block * inner + y, rows, :].astype(jnp.float32)
            for d in range(1, inner):
                total += from_y[d - 1, dz, rows, :].astype(jnp.float32)
            sum_y[dz, rows, :] = total.astype(sum_y.dtype)

        if dz:
            copy = remote(sum_y.at[dz], from_z.at[dz - 1], zsem.at[dz - 1], zrec.at[dz - 1], gx_at(z_at(dz)))
            copy.start()
            z_copies.append(copy)
    for copy in z_copies:
        copy.wait_recv()

    @pl.loop(0, samples // step)
    def _(i):
        rows = pl.ds(pl.multiple_of(i * step, step), step)
        total = sum_y[0, rows, :].astype(jnp.float32)
        for d in range(1, outer):
            total += from_z[d - 1, rows, :].astype(jnp.float32)
        feat[0, rows, :] = total.astype(feat.dtype)

    far = []
    for d in range(1, chips):
        copy = remote(feat.at[0], feat.at[2 * (chips - d)], gsem.at[d], grec.at[chips - d], gy_at(chip_at(d)))
        copy.start()
        far.append(copy)
    near = [remote(feat.at[0], feat.at[1], rsem.at[0], rrec.at[0], gy_at(partner))]
    near[0].start()
    for load in loads:
        load.wait()
    tile = 512
    hidden, outs = w_in.shape[1], w_out.shape[1]

    def scores(index, put):
        @pl.loop(0, hidden // tile)
        def _(i):
            cols = pl.ds(pl.multiple_of(i * tile, tile), tile)
            pre = jnp.dot(feat[index], w_in[:, cols], preferred_element_type=jnp.float32) + bias_ref[:, cols]
            hid[:, cols] = jnp.maximum(pre, 0.0).astype(hid.dtype)

        @pl.loop(0, outs // tile)
        def _(i):
            cols = pl.ds(pl.multiple_of(i * tile, tile), tile)
            put(cols, jnp.dot(hid[...], w_out[:, cols], preferred_element_type=jnp.float32))

    def to_partner(d):
        def put(cols, value):
            near_out[d, :, cols] = value.astype(near_out.dtype)

        scores(2 * d + 1, put)
        copy = remote(near_out.at[d], near_in.at[d], nsem.at[d], nrec.at[d], gy_at(partner))
        copy.start()
        return copy

    def kept(d):
        def put(cols, value):
            far_out[d, :, cols] = value

        scores(2 * d, put)

    last = []
    kept(0)
    near[0].wait_recv()
    last.append(to_partner(0))
    for d in range(1, chips):
        far[chips - 1 - d].wait_recv()
        copy = remote(feat.at[2 * d], feat.at[2 * d + 1], rsem.at[d], rrec.at[d], gy_at(partner))
        copy.start()
        near.append(copy)
        kept(d)
        copy.wait_recv()
        last.append(to_partner(d))
    far_copies = []
    for d in range(1, chips):
        last[d].wait_recv()

        @pl.loop(0, samples // step)
        def _(i):
            rows = pl.ds(pl.multiple_of(i * step, step), step)
            total = far_out[d, rows, :] + near_in[d, rows, :].astype(jnp.float32)
            w_send[d - 1, rows, :] = total.astype(w_send.dtype)

        copy = remote(w_send.at[d - 1], far_in.at[d - 1], fsem.at[d - 1], frec.at[d - 1], gy_at(chip_at(d)))
        copy.start()
        far_copies.append(copy)
    last[0].wait_recv()
    for copy in far_copies:
        copy.wait_recv()

    @pl.loop(0, samples // step)
    def _(i):
        rows = pl.ds(pl.multiple_of(i * step, step), step)
        total = far_out[0, rows, :] + near_in[0, rows, :].astype(jnp.float32)
        for d in range(1, chips):
            total += far_in[d - 1, rows, :].astype(jnp.float32)
        out_ref[rows, :] = total.astype(out_ref.dtype)

    for copy in sends + z_copies + far + near + last + far_copies:
        copy.wait_send()


def pool_kernel(samples, count, window, lo_ref, n_ref, keys_ref, table_ref, out_ref, tab, acc, smem, tsem, ksem):
    tables, rows_dev, emb = table_ref.shape
    sources = out_ref.shape[0]
    mask = rows_dev - 1
    shift = log2(rows_dev)
    segs = sources * tables

    def table_copy(t):
        return pltpu.make_async_copy(table_ref.at[t], tab.at[t % 2], tsem.at[t % 2])

    def key_copy(s, t, slot):
        start = (lo_ref[s, t] >> 10) << 10
        start = jnp.minimum(start, count - window)
        src = keys_ref.at[pl.ds(pl.multiple_of((s * tables + t) * count + start, 1024), window)]
        dst = smem.at[pl.ds(slot * window, window)]
        return pltpu.make_async_copy(src, dst, ksem.at[slot])

    trash = 2 * CHAINS * window
    for u in range(UNROLL):
        smem[trash + u] = samples * rows_dev
    steps = [(t, g) for t in range(tables) for g in range(sources // CHAINS)]

    def start_keys(index):
        t, g = steps[index]
        for j in range(CHAINS):
            key_copy(g * CHAINS + j, t, index % 2 * CHAINS + j).start()

    table_copy(0).start()
    start_keys(0)
    for index, (t, g) in enumerate(steps):
        if g == 0:
            if t + 1 < tables:
                table_copy(t + 1).start()
            table_copy(t).wait()
        if index + 1 < len(steps):
            start_keys(index + 1)
        acc[...] = jnp.zeros_like(acc)
        bases, ends, longest = [], [], 0
        for j in range(CHAINS):
            s = g * CHAINS + j
            slot = index % 2 * CHAINS + j
            key_copy(s, t, slot).wait()
            start = jnp.minimum((lo_ref[s, t] >> 10) << 10, count - window)
            first = ((lo_ref[s, t] - start) // UNROLL) * UNROLL
            bases.append(slot * window + first)
            ends.append(slot * window + lo_ref[s, t] - start + n_ref[s, t])
            longest = jnp.maximum(longest, ends[j] - bases[j])

        def body(i, carry):
            prevs, runs = list(carry[0]), list(carry[1])
            at = []
            for j in range(CHAINS):
                here = bases[j] + i * UNROLL
                at.append(jnp.where(here < ends[j], here, trash))
            for u in range(UNROLL):
                for j in range(CHAINS):
                    code = smem[at[j] + u]
                    bag = code >> shift
                    got = tab[t % 2, pl.ds(code & mask, 1), :]
                    runs[j] = jnp.where(bag == prevs[j], runs[j], 0.0) + got
                    acc[pl.ds(j * (samples + 8) + bag, 1), :] = runs[j]
                    prevs[j] = bag
            return tuple(prevs), tuple(runs)

        init = (
            tuple(jnp.int32(-1) for _ in range(CHAINS)),
            tuple(jnp.zeros((1, emb), jnp.float32) for _ in range(CHAINS)),
        )
        lax.fori_loop(0, (longest + UNROLL - 1) // UNROLL, body, init)
        for j in range(CHAINS):
            out_ref[g * CHAINS + j, :, t * emb : (t + 1) * emb] = acc[
                j * (samples + 8) : j * (samples + 8) + samples, :
            ].astype(out_ref.dtype)


def local(table, lookup_owner, lookup_row, bag_length, top_in, top_bias, top_out):
    owners = lax.axis_size("gx")
    me = lax.axis_index("gx")
    tables, samples, bag_size = lookup_row.shape
    rows_dev = table.shape[1]
    emb = table.shape[2]
    count = samples * bag_size
    cap = 2 * count // owners
    window = min(count, -(-cap // 1024) * 1024 + 1024)

    rows = tables * count // 128
    codes, counts = pl.pallas_call(
        functools.partial(sort_kernel, rows_dev),
        out_shape=(
            jax.ShapeDtypeStruct((owners, rows, 128), jnp.int32),
            jax.ShapeDtypeStruct((2, owners, tables, 8, 128), jnp.int32),
        ),
        scratch_shapes=[
            pltpu.VMEM((rows, 128), jnp.int32),
            pltpu.VMEM((owners, rows, 128), jnp.int32),
            pltpu.SemaphoreType.DMA((owners,)),
            pltpu.SemaphoreType.DMA((owners,)),
        ],
        compiler_params=pltpu.CompilerParams(collective_id=0, has_side_effects=True),
        name="sort_keys",
    )(
        jnp.transpose(lookup_owner[..., 0], (0, 2, 1)),
        jnp.transpose(lookup_row, (0, 2, 1)),
        bag_length[:, None, :],
    )
    totals = jnp.sum(counts, axis=(3, 4))
    lo, number = totals[0], totals[1]
    partial = pl.pallas_call(
        functools.partial(pool_kernel, samples, count, window),
        out_shape=jax.ShapeDtypeStruct((owners, samples, tables * emb), jnp.bfloat16),
        in_specs=[
            pl.BlockSpec(memory_space=pltpu.SMEM),
            pl.BlockSpec(memory_space=pltpu.SMEM),
            pl.BlockSpec(memory_space=pl.ANY),
            pl.BlockSpec(memory_space=pl.ANY),
        ],
        scratch_shapes=[
            pltpu.VMEM((2, rows_dev, emb), jnp.float32),
            pltpu.VMEM((CHAINS * (samples + 8), emb), jnp.float32),
            pltpu.SMEM((2 * CHAINS * window + 128,), jnp.int32),
            pltpu.SemaphoreType.DMA((2,)),
            pltpu.SemaphoreType.DMA((2 * CHAINS,)),
        ],
        name="pool",
    )(lo, number, codes.reshape(-1), table)
    inner = max(1, owners // 4)
    outer = owners // inner
    chips = lax.axis_size("gy") // 2
    width = tables * emb
    hidden, outs = top_out.shape
    bf16, dma = jnp.bfloat16, pltpu.SemaphoreType.DMA
    vmem = pl.BlockSpec(memory_space=pltpu.VMEM)
    return pl.pallas_call(
        exchange_kernel,
        out_shape=jax.ShapeDtypeStruct((samples, outs), bf16),
        in_specs=[vmem, pl.BlockSpec(memory_space=pl.ANY), vmem, pl.BlockSpec(memory_space=pl.ANY)],
        out_specs=vmem,
        scratch_shapes=[
            pltpu.VMEM((inner - 1, outer, samples, width), bf16),
            pltpu.VMEM((outer, samples, width), bf16),
            pltpu.VMEM((outer - 1, samples, width), bf16),
            pltpu.VMEM((2 * chips, samples, width), bf16),
            pltpu.VMEM((width, hidden), bf16),
            pltpu.VMEM((hidden, outs), bf16),
            pltpu.VMEM((samples, hidden), bf16),
            pltpu.VMEM((chips, samples, outs), bf16),
            pltpu.VMEM((chips, samples, outs), bf16),
            pltpu.VMEM((chips, samples, outs), jnp.float32),
            pltpu.VMEM((chips - 1, samples, outs), bf16),
            pltpu.VMEM((chips - 1, samples, outs), bf16),
            dma((2,)),
            dma((inner - 1, outer)),
            dma((inner - 1, outer)),
            dma((outer - 1,)),
            dma((outer - 1,)),
            dma((chips,)),
            dma((chips,)),
            dma((chips,)),
            dma((chips,)),
            dma((chips,)),
            dma((chips,)),
            dma((chips - 1,)),
            dma((chips - 1,)),
        ],
        compiler_params=pltpu.CompilerParams(
            collective_id=1, has_side_effects=True, vmem_limit_bytes=50 * 2**20
        ),
        name="exchange",
    )(partial, top_in, top_bias[None, :], top_out)


def solution(mesh):
    return jax.shard_map(
        local,
        mesh=mesh,
        in_specs=(
            P(None, "gx", None),
            P(None, ("gx", "gy"), None, None),
            P(None, ("gx", "gy"), None),
            P(None, ("gx", "gy")),
            P(None, "gy"),
            P("gy"),
            P("gy", None),
        ),
        out_specs=P(("gx", "gy"), None),
        check_vma=False,
    )
```

```python
import functools
import jax
import jax.numpy as jnp
from jax import lax
from jax.experimental import pallas as pl
from jax.experimental.pallas import tpu as pltpu
from jax.sharding import PartitionSpec as P

UNROLL = 8
CHAINS = 4
BIG = 2**31 - 1
MESH = pl.DeviceIdType.MESH


def log2(n):
    return n.bit_length() - 1


def sort_kernel(rows_dev, owner_ref, row_ref, bag_ref, codes_ref, count_ref, mine, held, send_sem, recv_sem):
    owners = held.shape[0]
    me = lax.axis_index("gx")
    barrier = pltpu.get_barrier_semaphore()
    for k in range(1, owners):
        pl.semaphore_signal(barrier, inc=1, device_id={"gx": lax.rem(me + k, owners)}, device_id_type=MESH)
    tables, bag_size, samples = owner_ref.shape
    owner = owner_ref[...]
    slot = lax.broadcasted_iota(jnp.int32, owner.shape, 1)
    sample = lax.broadcasted_iota(jnp.int32, owner.shape, 2)
    live = slot < bag_ref[...][:, None, :]
    key = jnp.where(live, (owner * samples + sample) * rows_dev + row_ref[...], BIG)
    count = bag_size * samples
    groups = count // 1024
    parts = []
    for t in range(tables):
        for c in range(samples // 128):
            for r in range(bag_size // 8):
                parts.append(key[t, r * 8 : r * 8 + 8, c * 128 : c * 128 + 128])
    lane = lax.broadcasted_iota(jnp.int32, (8, 128), 1)
    sub = lax.broadcasted_iota(jnp.int32, (8, 128), 0)
    place = sub * 128 + lane
    bits = log2(count)
    for k in range(1, bits + 1):
        for j in range(k - 1, -1, -1):
            d = 1 << j
            new = [None] * len(parts)
            for v in range(len(parts)):
                g = v % groups
                if d >= 1024:
                    gd = d // 1024
                    if g & gd:
                        continue
                    w = v + gd
                    low = jnp.minimum(parts[v], parts[w])
                    high = jnp.maximum(parts[v], parts[w])
                    up = ((g * 1024) >> k) & 1 == 0
                    new[v], new[w] = (low, high) if up else (high, low)
                    continue
                x = parts[v]
                if d < 128:
                    a, b = pltpu.roll(x, 128 - d, 1), pltpu.roll(x, d, 1)
                else:
                    s = d // 128
                    a, b = pltpu.roll(x, 8 - s, 0), pltpu.roll(x, s, 0)
                first = (place & d) == 0
                other = jnp.where(first, a, b)
                if (1 << k) >= 1024:
                    up = ((g * 1024) >> k) & 1 == 0
                    take_low = first if up else jnp.logical_not(first)
                else:
                    take_low = ((place >> k) ^ (place >> j)) & 1 == 0
                new[v] = jnp.where(take_low, jnp.minimum(x, other), jnp.maximum(x, other))
            parts = new
    for v in range(len(parts)):
        mine[v * 8 : v * 8 + 8, :] = parts[v]
    pl.semaphore_wait(barrier, owners - 1)
    copies = []
    for k in range(1, owners):
        copies.append(
            pltpu.make_async_remote_copy(
                src_ref=mine,
                dst_ref=held.at[me],
                send_sem=send_sem.at[k],
                recv_sem=recv_sem.at[k],
                device_id={"gx": lax.rem(me + k, owners)},
                device_id_type=MESH,
            )
        )
        copies[-1].start()
    span = samples * rows_dev
    base = me * span

    def recode(source, get):
        for t in range(tables):
            before = jnp.zeros((8, 128), jnp.int32)
            inside = jnp.zeros((8, 128), jnp.int32)
            for g in range(groups):
                at = (t * groups + g) * 8
                x = get(at) - base
                early = x < 0
                ours = jnp.logical_and(x >= 0, x < span)
                codes_ref[source, at : at + 8, :] = jnp.where(ours, x, span)
                before += early.astype(jnp.int32)
                inside += ours.astype(jnp.int32)
            at = source * tables + t
            count_ref[pl.ds(at, 1), :] = jnp.sum(before, axis=0, keepdims=True)
            count_ref[pl.ds(owners * tables + at, 1), :] = jnp.sum(inside, axis=0, keepdims=True)

    recode(me, lambda at: mine[at : at + 8, :])
    for k in range(1, owners):
        source = lax.rem(me - k + owners, owners)
        copies[k - 1].wait_recv()
        recode(source, lambda at: held[source, at : at + 8, :])
    for copy in copies:
        copy.wait_send()


def exchange_kernel(part_ref, top_in_ref, bias_ref, top_out_ref, out_ref, from_y, sum_y, from_z, feat, w_in, w_out, hid, near_out, near_in, far_out, w_send, far_in, wsem, ysem, yrec, zsem, zrec, gsem, grec, rsem, rrec, nsem, nrec, fsem, frec):
    owners, samples, width = part_ref.shape
    inner = from_y.shape[0] + 1
    outer = owners // inner
    chips = far_in.shape[0] + 1
    me, mine = lax.axis_index("gx"), lax.axis_index("gy")
    z, y = me // inner, lax.rem(me, inner)
    chip, core = mine // 2, lax.rem(mine, 2)
    partner = chip * 2 + 1 - core
    loads = [
        pltpu.make_async_copy(top_in_ref, w_in, wsem.at[0]),
        pltpu.make_async_copy(top_out_ref, w_out, wsem.at[1]),
    ]
    for load in loads:
        load.start()

    def gx_at(index):
        return {"gx": index}

    def gy_at(index):
        return {"gy": index}

    def remote(src, dst, send, recv, device):
        return pltpu.make_async_remote_copy(
            src_ref=src, dst_ref=dst, send_sem=send, recv_sem=recv, device_id=device, device_id_type=MESH
        )

    def y_at(d):
        return z * inner + lax.rem(y + d, inner)

    def z_at(d):
        return lax.rem(z + d, outer) * inner + y

    def chip_at(d):
        return lax.rem(chip + d, chips) * 2 + core

    peers = [gx_at(y_at(d)) for d in range(1, inner)]
    peers += [gx_at(z_at(d)) for d in range(1, outer)]
    peers += [gy_at(partner)] + [gy_at(chip_at(d)) for d in range(1, chips)]
    barrier = pltpu.get_barrier_semaphore()
    for peer in peers:
        pl.semaphore_signal(barrier, inc=1, device_id=peer, device_id_type=MESH)
    pl.semaphore_wait(barrier, len(peers))

    sends = []
    order = sorted(range(1, outer), key=lambda d: -min(d, outer - d)) + [0]
    y_copies = {}
    for dz in order:
        for d in range(1, inner):
            block = lax.rem(z + dz, outer)
            copy = remote(
                part_ref.at[block * inner + lax.rem(y + d, inner)],
                from_y.at[d - 1, dz],
                ysem.at[d - 1, dz],
                yrec.at[d - 1, dz],
                gx_at(y_at(d)),
            )
            copy.start()
            y_copies[dz, d] = copy
            sends.append(copy)
    step = 64
    z_copies = []
    for dz in order:
        block = lax.rem(z + dz, outer)
        for d in range(1, inner):
            y_copies[dz, d].wait_recv()

        @pl.loop(0, samples // step)
        def _(i):
            rows = pl.ds(pl.multiple_of(i * step, step), step)
            total = part_ref[block * inner + y, rows, :].astype(jnp.float32)
            for d in range(1, inner):
                total += from_y[d - 1, dz, rows, :].astype(jnp.float32)
            sum_y[dz, rows, :] = total.astype(sum_y.dtype)

        if dz:
            copy = remote(sum_y.at[dz], from_z.at[dz - 1], zsem.at[dz - 1], zrec.at[dz - 1], gx_at(z_at(dz)))
            copy.start()
            z_copies.append(copy)
    for copy in z_copies:
        copy.wait_recv()

    @pl.loop(0, samples // step)
    def _(i):
        rows = pl.ds(pl.multiple_of(i * step, step), step)
        total = sum_y[0, rows, :].astype(jnp.float32)
        for d in range(1, outer):
            total += from_z[d - 1, rows, :].astype(jnp.float32)
        feat[0, rows, :] = total.astype(feat.dtype)

    far = []
    for d in range(1, chips):
        copy = remote(feat.at[0], feat.at[2 * (chips - d)], gsem.at[d], grec.at[chips - d], gy_at(chip_at(d)))
        copy.start()
        far.append(copy)
    near = [remote(feat.at[0], feat.at[1], rsem.at[0], rrec.at[0], gy_at(partner))]
    near[0].start()
    for load in loads:
        load.wait()
    tile = 512
    hidden, outs = w_in.shape[1], w_out.shape[1]

    def scores(index, put):
        @pl.loop(0, hidden // tile)
        def _(i):
            cols = pl.ds(pl.multiple_of(i * tile, tile), tile)
            pre = jnp.dot(feat[index], w_in[:, cols], preferred_element_type=jnp.float32) + bias_ref[:, cols]
            hid[:, cols] = jnp.maximum(pre, 0.0).astype(hid.dtype)

        @pl.loop(0, outs // tile)
        def _(i):
            cols = pl.ds(pl.multiple_of(i * tile, tile), tile)
            put(cols, jnp.dot(hid[...], w_out[:, cols], preferred_element_type=jnp.float32))

    def to_partner(d):
        def put(cols, value):
            near_out[d, :, cols] = value.astype(near_out.dtype)

        scores(2 * d + 1, put)
        copy = remote(near_out.at[d], near_in.at[d], nsem.at[d], nrec.at[d], gy_at(partner))
        copy.start()
        return copy

    def kept(d):
        def put(cols, value):
            far_out[d, :, cols] = value

        scores(2 * d, put)

    last = []
    kept(0)
    near[0].wait_recv()
    last.append(to_partner(0))
    for d in range(1, chips):
        far[chips - 1 - d].wait_recv()
        copy = remote(feat.at[2 * d], feat.at[2 * d + 1], rsem.at[d], rrec.at[d], gy_at(partner))
        copy.start()
        near.append(copy)
        kept(d)
        copy.wait_recv()
        last.append(to_partner(d))
    far_copies = []
    for d in range(1, chips):
        last[d].wait_recv()

        @pl.loop(0, samples // step)
        def _(i):
            rows = pl.ds(pl.multiple_of(i * step, step), step)
            total = far_out[d, rows, :] + near_in[d, rows, :].astype(jnp.float32)
            w_send[d - 1, rows, :] = total.astype(w_send.dtype)

        copy = remote(w_send.at[d - 1], far_in.at[d - 1], fsem.at[d - 1], frec.at[d - 1], gy_at(chip_at(d)))
        copy.start()
        far_copies.append(copy)
    last[0].wait_recv()
    for copy in far_copies:
        copy.wait_recv()

    @pl.loop(0, samples // step)
    def _(i):
        rows = pl.ds(pl.multiple_of(i * step, step), step)
        total = far_out[0, rows, :] + near_in[0, rows, :].astype(jnp.float32)
        for d in range(1, chips):
            total += far_in[d - 1, rows, :].astype(jnp.float32)
        out_ref[rows, :] = total.astype(out_ref.dtype)

    for copy in sends + z_copies + far + near + last + far_copies:
        copy.wait_send()


def pool_kernel(samples, count, window, totals_ref, keys_ref, table_ref, out_ref, tab, acc, smem, tsem, ksem):
    tables, rows_dev, emb = table_ref.shape
    sources = out_ref.shape[0]
    mask = rows_dev - 1
    shift = log2(rows_dev)
    segs = sources * tables

    def table_copy(t):
        return pltpu.make_async_copy(table_ref.at[t], tab.at[t % 2], tsem.at[t % 2])

    def key_copy(s, t, slot):
        start = (totals_ref[s * tables + t] >> 10) << 10
        start = jnp.minimum(start, count - window)
        src = keys_ref.at[pl.ds(pl.multiple_of((s * tables + t) * count + start, 1024), window)]
        dst = smem.at[pl.ds(slot * window, window)]
        return pltpu.make_async_copy(src, dst, ksem.at[slot])

    trash = 2 * CHAINS * window
    for u in range(UNROLL):
        smem[trash + u] = samples * rows_dev
    steps = [(t, g) for t in range(tables) for g in range(sources // CHAINS)]

    def start_keys(index):
        t, g = steps[index]
        for j in range(CHAINS):
            key_copy(g * CHAINS + j, t, index % 2 * CHAINS + j).start()

    table_copy(0).start()
    start_keys(0)
    for index, (t, g) in enumerate(steps):
        if g == 0:
            if t + 1 < tables:
                table_copy(t + 1).start()
            table_copy(t).wait()
        if index + 1 < len(steps):
            start_keys(index + 1)
        acc[...] = jnp.zeros_like(acc)
        bases, ends, longest = [], [], 0
        for j in range(CHAINS):
            s = g * CHAINS + j
            slot = index % 2 * CHAINS + j
            key_copy(s, t, slot).wait()
            start = jnp.minimum((totals_ref[s * tables + t] >> 10) << 10, count - window)
            first = ((totals_ref[s * tables + t] - start) // UNROLL) * UNROLL
            bases.append(slot * window + first)
            ends.append(slot * window + totals_ref[s * tables + t] - start + totals_ref[segs + s * tables + t])
            longest = jnp.maximum(longest, ends[j] - bases[j])

        def body(i, carry):
            prevs, runs = list(carry[0]), list(carry[1])
            at = []
            for j in range(CHAINS):
                here = bases[j] + i * UNROLL
                at.append(jnp.where(here < ends[j], here, trash))
            for u in range(UNROLL):
                for j in range(CHAINS):
                    code = smem[at[j] + u]
                    got = tab[t % 2, pl.ds(code & mask, 1), :]
                    bags = jnp.full((1, emb), code, jnp.int32) >> shift
                    runs[j] = jnp.where(bags == prevs[j], runs[j], 0.0) + got
                    acc[pl.ds(j * (samples + 8) + (code >> shift), 1), :] = runs[j]
                    prevs[j] = bags
            return tuple(prevs), tuple(runs)

        init = (
            tuple(jnp.full((1, emb), -1, jnp.int32) for _ in range(CHAINS)),
            tuple(jnp.zeros((1, emb), jnp.float32) for _ in range(CHAINS)),
        )
        lax.fori_loop(0, (longest + UNROLL - 1) // UNROLL, body, init)
        for j in range(CHAINS):
            out_ref[g * CHAINS + j, :, t * emb : (t + 1) * emb] = acc[
                j * (samples + 8) : j * (samples + 8) + samples, :
            ].astype(out_ref.dtype)


def local(table, lookup_owner, lookup_row, bag_length, top_in, top_bias, top_out):
    owners = lax.axis_size("gx")
    me = lax.axis_index("gx")
    tables, samples, bag_size = lookup_row.shape
    rows_dev = table.shape[1]
    emb = table.shape[2]
    count = samples * bag_size
    cap = 2 * count // owners
    window = min(count, -(-cap // 1024) * 1024 + 1024)

    rows = tables * count // 128
    codes, counts = pl.pallas_call(
        functools.partial(sort_kernel, rows_dev),
        out_shape=(
            jax.ShapeDtypeStruct((owners, rows, 128), jnp.int32),
            jax.ShapeDtypeStruct((2 * owners * tables, 128), jnp.int32),
        ),
        scratch_shapes=[
            pltpu.VMEM((rows, 128), jnp.int32),
            pltpu.VMEM((owners, rows, 128), jnp.int32),
            pltpu.SemaphoreType.DMA((owners,)),
            pltpu.SemaphoreType.DMA((owners,)),
        ],
        compiler_params=pltpu.CompilerParams(collective_id=0, has_side_effects=True),
        name="sort_keys",
    )(
        jnp.transpose(lookup_owner[..., 0], (0, 2, 1)),
        jnp.transpose(lookup_row, (0, 2, 1)),
        bag_length,
    )
    totals = jnp.sum(counts, axis=1)
    partial = pl.pallas_call(
        functools.partial(pool_kernel, samples, count, window),
        out_shape=jax.ShapeDtypeStruct((owners, samples, tables * emb), jnp.bfloat16),
        in_specs=[
            pl.BlockSpec(memory_space=pltpu.SMEM),
            pl.BlockSpec(memory_space=pl.ANY),
            pl.BlockSpec(memory_space=pl.ANY),
        ],
        scratch_shapes=[
            pltpu.VMEM((2, rows_dev, emb), jnp.float32),
            pltpu.VMEM((CHAINS * (samples + 8), emb), jnp.float32),
            pltpu.SMEM((2 * CHAINS * window + 128,), jnp.int32),
            pltpu.SemaphoreType.DMA((2,)),
            pltpu.SemaphoreType.DMA((2 * CHAINS,)),
        ],
        name="pool",
    )(totals, codes.reshape(-1), table)
    inner = max(1, owners // 4)
    outer = owners // inner
    chips = lax.axis_size("gy") // 2
    width = tables * emb
    hidden, outs = top_out.shape
    bf16, dma = jnp.bfloat16, pltpu.SemaphoreType.DMA
    vmem = pl.BlockSpec(memory_space=pltpu.VMEM)
    return pl.pallas_call(
        exchange_kernel,
        out_shape=jax.ShapeDtypeStruct((samples, outs), bf16),
        in_specs=[vmem, pl.BlockSpec(memory_space=pl.ANY), vmem, pl.BlockSpec(memory_space=pl.ANY)],
        out_specs=vmem,
        scratch_shapes=[
            pltpu.VMEM((inner - 1, outer, samples, width), bf16),
            pltpu.VMEM((outer, samples, width), bf16),
            pltpu.VMEM((outer - 1, samples, width), bf16),
            pltpu.VMEM((2 * chips, samples, width), bf16),
            pltpu.VMEM((width, hidden), bf16),
            pltpu.VMEM((hidden, outs), bf16),
            pltpu.VMEM((samples, hidden), bf16),
            pltpu.VMEM((chips, samples, outs), bf16),
            pltpu.VMEM((chips, samples, outs), bf16),
            pltpu.VMEM((chips, samples, outs), jnp.float32),
            pltpu.VMEM((chips - 1, samples, outs), bf16),
            pltpu.VMEM((chips - 1, samples, outs), bf16),
            dma((2,)),
            dma((inner - 1, outer)),
            dma((inner - 1, outer)),
            dma((outer - 1,)),
            dma((outer - 1,)),
            dma((chips,)),
            dma((chips,)),
            dma((chips,)),
            dma((chips,)),
            dma((chips,)),
            dma((chips,)),
            dma((chips - 1,)),
            dma((chips - 1,)),
        ],
        compiler_params=pltpu.CompilerParams(
            collective_id=1, has_side_effects=True, vmem_limit_bytes=50 * 2**20
        ),
        name="exchange",
    )(partial, top_in, top_bias[None, :], top_out)


def solution(mesh):
    return jax.shard_map(
        local,
        mesh=mesh,
        in_specs=(
            P(None, "gx", None),
            P(None, ("gx", "gy"), None, None),
            P(None, ("gx", "gy"), None),
            P(None, ("gx", "gy")),
            P(None, "gy"),
            P("gy"),
            P("gy", None),
        ),
        out_specs=P(("gx", "gy"), None),
        check_vma=False,
    )
```
